32 devices in a mesh: grp: 2 (over y), var: 8 (over z, x), smp: 2 (over core).
Axes of the slice: x: 2, y: 2, z: 4, core: 2. Of those that a mesh axis runs over, the one named last changes fastest.
Arguments:
- genotypes: bfloat16 [15360, 1024], P(('grp', 'smp'), 'var'), parts along dimension 0, may hold values from 0 to 2, as said below
- ancestry_counts: int32 [15360, 32], P(('grp', 'smp')), parts along dimension 0, may hold values from 1 to 100
- residuals: int32 [15360, 16], P(('grp', 'smp')), parts along dimension 0, may hold values from -3000 to 3000
- freqs: float32 [64, 1024], P('grp', 'var'), parts along dimension 0, may hold values from 0.05 to 0.95
Outputs:
- q_new: float32 [15360, 32], P(('grp', 'smp', 'var')), parts along dimension 0
- q_gradient: float32 [15360, 32], P(('grp', 'smp', 'var')), parts along dimension 0
- p_new: float32 [64, 1024], P('grp', 'var'), parts along dimension 0
- p_gradient: float32 [64, 1024], P('grp', 'var'), parts along dimension 0
- z_score: float32 [64, 16, 1024], P('grp', None, 'var'), parts along dimension 0
The draws below stay inside these ranges and needn't reach their ends.
There are 2 independent parts, one for each index of `grp`. The reference program is written for one: setup_inputs(seed, part) draws one part's arguments, and reference() takes and returns one part's arrays. A program takes and returns all parts, laid end to end along the dimension named above; each array names one. Nothing has to cross between parts.
Inputs may be any that keep to these rules, and one draw needn't show every extreme that they name: `genotypes`: dosages lie in the closed range from 0 to 2.
All inputs are finite; a program needn't handle non-finite values.
Results may differ from the reference program's by a relative error of at most 0.0003.
Values sent between devices are 32-bit elements; how exact they have to be, the bound alone decides.
A program may use at most 64 MiB of HBM per device.

```python
import math
import jax
import jax.numpy as jnp
from jax import lax

ANC = 32
TRAITS = 16
MV = 128
SAMPLES = 7680
VARIANTS = 1024
N_VAR = 8


def draw_genotypes(key, part):
    logits = jax.random.uniform(jax.random.fold_in(key, 11), (1, VARIANTS), jnp.float32, -2.5, 2.5)
    block_rows = 960
    block_ids = jnp.arange(SAMPLES // block_rows, dtype=jnp.int32)

    def one_block(block_index):
        block_key = jax.random.fold_in(jax.random.fold_in(key, 12), block_index)
        first_key, second_key = jax.random.split(block_key)
        noise_one = 2.0 * jax.random.normal(first_key, (block_rows, VARIANTS), jnp.float32)
        noise_two = 2.0 * jax.random.normal(second_key, (block_rows, VARIANTS), jnp.float32)
        dosage = jax.nn.sigmoid(logits + noise_one) + jax.nn.sigmoid(logits + noise_two)
        return dosage
    blocks = lax.map(one_block, block_ids)
    return blocks.reshape(SAMPLES, VARIANTS).astype(jnp.bfloat16)


def with_ends(array, key, low, largest):
    longest = array.shape.index(max(array.shape))
    spots = []
    for shift in (0, 1):
        where = [jax.random.randint(jax.random.fold_in(key, axis), (), 0, length) for axis, length in enumerate(array.shape)]
        where[longest] = (where[longest] + shift) % array.shape[longest]
        spots.append(tuple(where))
    return array.at[spots[0]].set(low).at[spots[1]].set(largest)


def levels(own_key, dims, pieces, least, top_value):
    gain = 1.0
    for axis_at, shards_of in pieces:
        steps = jax.random.uniform(jax.random.fold_in(jax.random.fold_in(own_key, 6), axis_at), (shards_of,), jnp.float32, least / len(pieces), top_value / len(pieces))
        gain = gain * jnp.repeat(jnp.exp(steps), dims[axis_at] // shards_of).reshape((-1,) + (1,) * (len(dims) - 1 - axis_at))
    return gain


def setup_inputs(seed: int = 0, part: int = 0) -> dict:
    splits = jax.random.split(jax.random.key(seed), 5)
    own_keys = jax.random.split(jax.random.fold_in(splits[4], part), 5)
    return {
        "genotypes": draw_genotypes(jax.random.fold_in(jax.random.fold_in(splits[4], part), 71), part),
        "ancestry_counts": with_ends(jax.random.randint(own_keys[1], (SAMPLES, ANC), 1, 101), jax.random.fold_in(own_keys[1], 1), 1, 100).astype(jnp.int32),
        "residuals": with_ends(jax.random.randint(own_keys[2], (SAMPLES, TRAITS), -3000, 3001), jax.random.fold_in(own_keys[2], 1), -3000, 3000).astype(jnp.int32),
        "freqs": jnp.clip(0.05 + 0.9 * jax.random.uniform(own_keys[3], (ANC, VARIANTS), jnp.float32) ** levels(own_keys[3], (ANC, VARIANTS), ((1, 8),), -0.2, 0.2), 0.05, 0.95),
    }


def reference(genotypes, ancestry_counts, residuals, freqs):
    highest = lax.Precision.HIGHEST
    counts = ancestry_counts.astype(jnp.float32)
    fractions = counts / lax.optimization_barrier(jnp.sum(counts, axis=1, keepdims=True))
    residual = residuals.astype(jnp.float32) / 1000.0
    column_ids = jnp.arange(N_VAR, dtype=jnp.int32)

    def first_pass(state_pair, column):
        gradient, second = state_pair
        start = (column * MV).astype(jnp.int32)
        dosage = lax.dynamic_slice_in_dim(genotypes, start, MV, 1).astype(jnp.float32)
        freq_block = lax.dynamic_slice_in_dim(freqs, start, MV, 1)
        recon_block = jnp.dot(fractions, freq_block, precision=highest)
        ratio_a = dosage / recon_block
        ratio_b = (2.0 - dosage) / (1.0 - recon_block)
        excess = ratio_a - ratio_b
        gradient = gradient + jnp.dot(excess, freq_block.T, precision=highest)
        second = second + lax.optimization_barrier(jnp.sum(ratio_b, axis=1))
        excess_block = jnp.dot(fractions.T, excess, precision=highest)
        second_block = jnp.dot(fractions.T, ratio_b, precision=highest)
        return ((gradient, second), (excess_block, second_block))
    start_pair = (jnp.zeros((SAMPLES, ANC), jnp.float32), jnp.zeros((SAMPLES,), jnp.float32))
    (gradient, second), (excess_blocks, second_blocks) = lax.scan(first_pass, start_pair, column_ids)
    excess_sum = excess_blocks.transpose(1, 0, 2).reshape(ANC, VARIANTS)
    second_sum = second_blocks.transpose(1, 0, 2).reshape(ANC, VARIANTS)
    q_gradient = gradient / math.sqrt(VARIANTS)
    weighted = fractions * (gradient + second[:, None])
    q_new = weighted / lax.optimization_barrier(jnp.sum(weighted, axis=1, keepdims=True))
    allele_sum = excess_sum + second_sum
    p_new = freqs * allele_sum / (freqs * allele_sum + (1.0 - freqs) * second_sum)
    p_gradient = excess_sum * ANC / math.sqrt(SAMPLES)
    trait_rows = (q_new[:, :, None] * residual[:, None, :]).reshape(SAMPLES, ANC * TRAITS)
    squares = q_new * q_new

    def second_pass(state_pair, column):
        start = (column * MV).astype(jnp.int32)
        dosage = lax.dynamic_slice_in_dim(genotypes, start, MV, 1).astype(jnp.float32)
        freq_block = lax.dynamic_slice_in_dim(freqs, start, MV, 1)
        ratio_next = dosage / jnp.dot(q_new, freq_block, precision=highest)
        score_block = jnp.dot(trait_rows.T, ratio_next, precision=highest)
        info_block = jnp.dot(squares.T, ratio_next * ratio_next, precision=highest)
        return (state_pair, (score_block, info_block))
    _, (score_blocks, info_blocks) = lax.scan(second_pass, jnp.zeros((), jnp.float32), column_ids)
    score = score_blocks.transpose(1, 0, 2).reshape(ANC, TRAITS, VARIANTS)
    information = info_blocks.transpose(1, 0, 2).reshape(ANC, VARIANTS)
    z_score = score / jnp.sqrt(information + 1e-06)[:, None, :]
    return (q_new, q_gradient, p_new, p_gradient, z_score)
```

```python
import functools
import math

import jax
import jax.numpy as jnp
from jax import lax
from jax.experimental import pallas as pl
from jax.experimental.pallas import tpu as pltpu
from jax.sharding import PartitionSpec as P

MESH = pl.DeviceIdType.MESH
F32 = jnp.float32
BF16 = jnp.bfloat16


def normalize(fractions, gradient, second):
    weighted = fractions * (gradient + second[:, None])
    return weighted / jnp.sum(weighted, axis=1, keepdims=True)


def update_freqs(freqs, excess_sum, second_sum, sample_count):
    allele_sum = excess_sum + second_sum
    freq_next = freqs * allele_sum / (freqs * allele_sum + (1.0 - freqs) * second_sum)
    freq_gradient = excess_sum * freqs.shape[0] / math.sqrt(sample_count)
    return (freq_next, freq_gradient)


def shards_plain(genotypes, ancestry_counts, residuals, freqs):
    highest = lax.Precision.HIGHEST
    var_count = lax.axis_size("var")
    sample_rows = genotypes.shape[0]
    sample_count = sample_rows * lax.axis_size("smp")
    variant_count = genotypes.shape[1] * var_count
    anc_count = freqs.shape[0]
    trait_count = residuals.shape[1]
    counts = ancestry_counts.astype(jnp.float32)
    fractions = counts / jnp.sum(counts, axis=1, keepdims=True)
    dosage = genotypes.astype(jnp.float32)
    recon_rows = jnp.dot(fractions, freqs, precision=highest)
    ratio_a = dosage / recon_rows
    ratio_b = (2.0 - dosage) / (1.0 - recon_rows)
    excess = ratio_a - ratio_b
    gradient_part = jnp.dot(excess, freqs.T, precision=highest)
    second_part = jnp.sum(ratio_b, axis=1)
    excess_part = jnp.dot(fractions.T, excess, precision=highest)
    return_part = jnp.dot(fractions.T, ratio_b, precision=highest)
    share_rows = sample_rows // var_count
    first_row = lax.axis_index("var") * share_rows
    excess_sum, second_sum = lax.psum((excess_part, return_part), "smp")
    freq_next, freq_gradient = update_freqs(freqs, excess_sum, second_sum, sample_count)
    gradient_all, second_all = lax.psum((gradient_part, second_part), "var")
    fraction_next = normalize(fractions, gradient_all, second_all)
    own_next = lax.dynamic_slice_in_dim(fraction_next, first_row, share_rows, 0)
    own_gradient = lax.dynamic_slice_in_dim(gradient_all, first_row, share_rows, 0)
    scaled_gradient = own_gradient / math.sqrt(variant_count)
    ratio_next = dosage / jnp.dot(fraction_next, freqs, precision=highest)
    residual = residuals.astype(jnp.float32) / 1000.0
    trait_rows = (fraction_next[:, :, None] * residual[:, None, :]).reshape(
        sample_rows, anc_count * trait_count
    )
    score_part = jnp.dot(trait_rows.T, ratio_next, precision=highest)
    info_part = jnp.dot(
        (fraction_next * fraction_next).T, ratio_next * ratio_next, precision=highest
    )
    score_sum, info_sum = lax.psum((score_part, info_part), "smp")
    score_tiles = score_sum.reshape(anc_count, trait_count, genotypes.shape[1])
    z_score = score_tiles / jnp.sqrt(info_sum + 1e-06)[:, None, :]
    return (own_next, scaled_gradient, freq_next, freq_gradient, z_score)


def split(x):
    high = x.astype(BF16)
    return high, (x - high.astype(F32)).astype(BF16)


def dot(a, b):
    return jnp.dot(a, b, preferred_element_type=F32)


def dot_lanes(a, b):
    return lax.dot_general(a, b, (((1,), (1,)), ((), ())), preferred_element_type=F32)


def kernel(
    dims,
    geno, counts, resid, freqs,
    q_out, g_out, p_out, pg_out, z_out,
    dos, qf, gf, fcol, frow, ebuf, tbuf,
    acc_ex, acc_sc, acc_in,
    xs, xr, zs, zr, go, gp, fs, fr, ss, sr,
    xs_s, xs_r, zs_s, zs_r, za_s, za_r, xa_s, xa_r, f_s, f_r, s_s, s_r,
):
    chunks, width, half, zs_n, rows, variant_count, sample_count, share, var_n = dims
    anc = freqs.shape[0]
    traits = resid.shape[0]
    mv = freqs.shape[1]
    me = lax.axis_index("var")
    core = lax.axis_index("smp")
    x = lax.rem(me, 2)
    z = me // 2
    partner = {"var": z * 2 + (1 - x)}
    twin = {"smp": 1 - core}
    z_peers = [{"var": lax.rem(z + d, zs_n) * 2 + x} for d in range(1, zs_n)]

    barrier = pltpu.get_barrier_semaphore()
    for peer in [partner, twin] + z_peers:
        pl.semaphore_signal(barrier, inc=1, device_id=peer, device_id_type=MESH)

    p = freqs[...]
    p_hi, p_lo = split(p)
    stack = jnp.concatenate([p_hi.astype(F32), p_lo.astype(F32)] * 2, axis=0)
    fcol[...] = stack.T.astype(BF16)
    frow[0:anc, 0:mv] = p_hi
    frow[0:anc, mv:] = p_hi
    frow[anc:, 0:mv] = p_lo
    frow[anc:, mv:] = p_lo
    acc_ex[...] = jnp.zeros_like(acc_ex)
    acc_sc[...] = jnp.zeros_like(acc_sc)
    acc_in[...] = jnp.zeros_like(acc_in)

    def lanes(which, c):
        return pl.multiple_of(which * half + c * width, 128)

    def first_pass(off):
        d = geno[pl.ds(off, width), :].astype(F32).T
        dos[:, pl.ds(off, width)] = d.astype(BF16)
        c = counts[:, pl.ds(off, width)].astype(F32)
        total = jnp.sum(c, axis=0, keepdims=True)
        cb = c.astype(BF16)
        none = jnp.zeros_like(cb)
        u = dot(fcol[...], jnp.concatenate([cb, cb, none, none], axis=0))
        w = total - u
        inverse = 1.0 / (u * w)
        b = (2.0 - d) * u * inverse
        e = d * w * inverse - b
        e_hi, e_lo = split(e)
        b_hi, b_lo = split(b)
        ebuf[0:mv, :] = e_hi
        ebuf[mv : 2 * mv, :] = e_lo
        ebuf[2 * mv : 3 * mv, :] = b_hi
        ebuf[3 * mv :, :] = b_lo
        g = dot(frow[...], ebuf[0 : 2 * mv, :])
        acc_ex[...] += dot_lanes(ebuf[...], jnp.concatenate([cb] * (128 // anc), axis=0))
        return (g[0:anc, :] + g[anc:, :]) * total

    def second_pass(off, g):
        c = counts[:, pl.ds(off, width)].astype(F32)
        f = c / jnp.sum(c, axis=0, keepdims=True)
        second = 2.0 * variant_count - jnp.sum(f * g, axis=0, keepdims=True)
        weighted = f * (g + second)
        q = weighted / jnp.sum(weighted, axis=0, keepdims=True)
        qf[:, pl.ds(off, width)] = q
        gf[:, pl.ds(off, width)] = g * (1.0 / math.sqrt(variant_count))
        q_hi, q_lo = split(q)
        recon = dot(fcol[...], jnp.concatenate([q_hi, q_hi, q_lo, q_lo], axis=0))
        r = dos[:, pl.ds(off, width)].astype(F32) / recon
        r_hi, r_lo = split(r)
        s_hi, s_lo = split(r * r)
        t = resid[:, pl.ds(off, width)].astype(F32)
        for k in range(anc):
            t_hi, t_lo = split(q[k : k + 1, :] * t)
            tbuf[traits * k : traits * (k + 1), 0:width] = t_hi
            tbuf[traits * k : traits * (k + 1), width:] = t_lo
        r_cat = jnp.concatenate([r_hi, r_lo], axis=0)
        acc_sc[...] += dot_lanes(tbuf[...], jnp.concatenate([r_cat, r_cat], axis=1))
        y_hi, y_lo = split(q * q)
        none = jnp.zeros_like(y_hi)
        acc_in[...] += dot_lanes(
            jnp.concatenate([s_hi, s_lo], axis=0),
            jnp.concatenate([y_hi, y_lo, none, none], axis=0),
        )

    def copy(src, dst, send, recv, peer):
        return pltpu.make_async_remote_copy(
            src_ref=src, dst_ref=dst, send_sem=send, recv_sem=recv, device_id=peer, device_id_type=MESH
        )

    def x_reduce(c):
        return copy(xs.at[c], xr.at[c], xs_s.at[c], xs_r.at[c], partner)

    def z_reduce(c, d):
        to = pl.multiple_of(lax.rem(z + d, zs_n) * rows, 8)
        return copy(
            zs.at[c, pl.ds(to, rows), :], zr.at[c, d - 1], zs_s.at[c, d - 1], zs_r.at[c, d - 1], z_peers[d - 1]
        )

    mine = pl.multiple_of(z * rows, 8)

    def z_gather(c, d):
        piece = go.at[c, pl.ds(mine, rows), :]
        return copy(piece, piece, za_s.at[c, d - 1], za_r.at[c, d - 1], z_peers[d - 1])

    def z_gathered(c, d):
        source = pl.multiple_of(lax.rem(z + zs_n - d, zs_n) * rows, 8)
        piece = go.at[c, pl.ds(source, rows), :]
        return copy(piece, piece, za_s.at[c, d - 1], za_r.at[c, d - 1], z_peers[d - 1])

    def x_gather(c):
        return copy(go.at[c], gp.at[c], xa_s.at[c], xa_r.at[c], partner)

    pl.semaphore_wait(barrier, 2 + len(z_peers))

    def step_far(c, carry):
        xs[c] = first_pass(lanes(1 - x, c))
        x_reduce(c).start()
        return carry

    lax.fori_loop(0, chunks, step_far, 0)

    def step_near(c, carry):
        g = first_pass(lanes(x, c))
        x_reduce(c).wait_recv()
        zs[c] = g + xr[c]
        for d in range(1, zs_n):
            z_reduce(c, d).start()
        return carry

    lax.fori_loop(0, chunks, step_near, 0)

    ex = acc_ex[0:mv, :] + acc_ex[mv : 2 * mv, :]
    re = acc_ex[2 * mv : 3 * mv, :] + acc_ex[3 * mv :, :]
    fs[0:anc, :] = ex.T[0:anc, :]
    fs[anc:, :] = re.T[0:anc, :]
    freq_copy = copy(fs, fr, f_s, f_r, twin)
    freq_copy.start()

    def step_sum(c, carry):
        total = zs[c, pl.ds(mine, rows), :]
        for d in range(1, zs_n):
            z_reduce(c, d).wait_recv()
            total = total + zr[c, d - 1]
        go[c, pl.ds(mine, rows), :] = total
        for d in range(1, zs_n):
            z_gather(c, d).start()
        return carry

    lax.fori_loop(0, chunks, step_sum, 0)

    freq_copy.wait_recv()
    sums = fs[...] + fr[...]
    excess_sum = sums[0:anc, :]
    second_sum = sums[anc:, :]
    freq_next, freq_gradient = update_freqs(p, excess_sum, second_sum, sample_count)
    p_out[...] = freq_next
    pg_out[...] = freq_gradient

    def step_own(c, carry):
        for d in range(1, zs_n):
            z_gathered(c, d).wait_recv()
        x_gather(c).start()
        second_pass(lanes(x, c), go[c])
        return carry

    lax.fori_loop(0, chunks, step_own, 0)

    def step_other(c, carry):
        x_gather(c).wait_recv()
        second_pass(lanes(1 - x, c), gp[c])
        return carry

    lax.fori_loop(0, chunks, step_other, 0)

    tiles = anc * traits
    ss[0:tiles, :] = acc_sc[:, 0:mv] + acc_sc[:, mv:]
    info = (acc_in[0:mv, :] + acc_in[mv:, :]).T
    ss[tiles:, :] = info[0:anc, :] + info[anc : 2 * anc, :]
    score_copy = copy(ss, sr, s_s, s_r, twin)
    score_copy.start()

    for v in range(var_n):

        @pl.when(me == v)
        def _():
            q_out[...] = qf[:, share * v : share * (v + 1)]
            g_out[...] = gf[:, share * v : share * (v + 1)]

    def drain(c, carry):
        x_reduce(c).wait_send()
        x_gather(c).wait_send()
        for d in range(1, zs_n):
            z_reduce(c, d).wait_send()
            z_gather(c, d).wait_send()
        return carry

    lax.fori_loop(0, chunks, drain, 0)
    freq_copy.wait_send()
    score_copy.wait_recv()
    info_sum = ss[tiles:, :] + sr[tiles:, :]
    scale = 0.001 / jnp.sqrt(info_sum + 1e-06)
    for k in range(anc):
        at = slice(traits * k, traits * (k + 1))
        z_out[at, :] = (ss[at, :] + sr[at, :]) * scale[k : k + 1, :]
    score_copy.wait_send()


def fits(genotypes, residuals, freqs, var_n):
    samples, mv = genotypes.shape
    anc = freqs.shape[0]
    return (
        var_n == 8
        and lax.axis_size("smp") == 2
        and anc == 32
        and mv == 128
        and residuals.shape[1] % 16 == 0
        and samples % (2 * 128) == 0
        and samples % var_n == 0
    )


def shards(genotypes, ancestry_counts, residuals, freqs):
    var_n = lax.axis_size("var")
    if not fits(genotypes, residuals, freqs, var_n):
        return shards_plain(genotypes, ancestry_counts, residuals, freqs)
    samples, mv = genotypes.shape
    anc = freqs.shape[0]
    traits = residuals.shape[1]
    zs_n = var_n // 2
    rows = anc // zs_n
    half = samples // 2
    tiles = half // 128
    chunks = max(n for n in range(1, 6) if tiles % n == 0)
    width = half // chunks
    share = samples // var_n
    dims = (chunks, width, half, zs_n, rows, mv * var_n, samples * lax.axis_size("smp"), share, var_n)
    vmem = pl.BlockSpec(memory_space=pltpu.VMEM)
    dma = pltpu.SemaphoreType.DMA
    part = pltpu.VMEM((chunks, anc, width), F32)
    q_t, g_t, p_new, p_grad, z_flat = pl.pallas_call(
        functools.partial(kernel, dims),
        out_shape=(
            jax.ShapeDtypeStruct((anc, share), F32),
            jax.ShapeDtypeStruct((anc, share), F32),
            jax.ShapeDtypeStruct((anc, mv), F32),
            jax.ShapeDtypeStruct((anc, mv), F32),
            jax.ShapeDtypeStruct((anc * traits, mv), F32),
        ),
        in_specs=[vmem] * 4,
        out_specs=(vmem,) * 5,
        scratch_shapes=[
            pltpu.VMEM((mv, samples), BF16),
            pltpu.VMEM((anc, samples), F32),
            pltpu.VMEM((anc, samples), F32),
            pltpu.VMEM((mv, 4 * anc), BF16),
            pltpu.VMEM((2 * anc, 2 * mv), BF16),
            pltpu.VMEM((4 * mv, width), BF16),
            pltpu.VMEM((anc * traits, 2 * width), BF16),
            pltpu.VMEM((4 * mv, 128), F32),
            pltpu.VMEM((anc * traits, 2 * mv), F32),
            pltpu.VMEM((2 * mv, 128), F32),
            part, part, part,
            pltpu.VMEM((chunks, zs_n - 1, rows, width), F32),
            part, part,
            pltpu.VMEM((2 * anc, mv), F32),
            pltpu.VMEM((2 * anc, mv), F32),
            pltpu.VMEM((anc * traits + anc, mv), F32),
            pltpu.VMEM((anc * traits + anc, mv), F32),
            dma((chunks,)), dma((chunks,)),
            dma((chunks, zs_n - 1)), dma((chunks, zs_n - 1)),
            dma((chunks, zs_n - 1)), dma((chunks, zs_n - 1)),
            dma((chunks,)), dma((chunks,)),
            dma, dma, dma, dma,
        ],
        compiler_params=pltpu.CompilerParams(collective_id=0, has_side_effects=True),
        name="em_step",
    )(genotypes, ancestry_counts.T, residuals.T, freqs)
    return (q_t.T, g_t.T, p_new, p_grad, z_flat.reshape(anc, traits, mv))


def solution(mesh):
    in_specs = (
        P(("grp", "smp"), "var"),
        P(("grp", "smp"), None),
        P(("grp", "smp"), None),
        P("grp", "var"),
    )
    out_specs = (
        P(("grp", "smp", "var"), None),
        P(("grp", "smp", "var"), None),
        P("grp", "var"),
        P("grp", "var"),
        P("grp", None, "var"),
    )
    return jax.shard_map(shards, mesh=mesh, in_specs=in_specs, out_specs=out_specs, check_vma=False)
```

```python
import functools
import math

import jax
import jax.numpy as jnp
from jax import lax
from jax.experimental import pallas as pl
from jax.experimental.pallas import tpu as pltpu
from jax.sharding import PartitionSpec as P

MESH = pl.DeviceIdType.MESH
F32 = jnp.float32
BF16 = jnp.bfloat16
LIMIT = 67043328 - 491520
MOST = 5


def normalize(fractions, gradient, second):
    weighted = fractions * (gradient + second[:, None])
    return weighted / jnp.sum(weighted, axis=1, keepdims=True)


def update_freqs(freqs, excess_sum, second_sum, sample_count):
    allele_sum = excess_sum + second_sum
    freq_next = freqs * allele_sum / (freqs * allele_sum + (1.0 - freqs) * second_sum)
    freq_gradient = excess_sum * freqs.shape[0] / math.sqrt(sample_count)
    return (freq_next, freq_gradient)


def shards_plain(genotypes, ancestry_counts, residuals, freqs):
    highest = lax.Precision.HIGHEST
    var_count = lax.axis_size("var")
    sample_rows = genotypes.shape[0]
    sample_count = sample_rows * lax.axis_size("smp")
    variant_count = genotypes.shape[1] * var_count
    anc_count = freqs.shape[0]
    trait_count = residuals.shape[1]
    counts = ancestry_counts.astype(jnp.float32)
    fractions = counts / jnp.sum(counts, axis=1, keepdims=True)
    dosage = genotypes.astype(jnp.float32)
    recon_rows = jnp.dot(fractions, freqs, precision=highest)
    ratio_a = dosage / recon_rows
    ratio_b = (2.0 - dosage) / (1.0 - recon_rows)
    excess = ratio_a - ratio_b
    gradient_part = jnp.dot(excess, freqs.T, precision=highest)
    second_part = jnp.sum(ratio_b, axis=1)
    excess_part = jnp.dot(fractions.T, excess, precision=highest)
    return_part = jnp.dot(fractions.T, ratio_b, precision=highest)
    share_rows = sample_rows // var_count
    first_row = lax.axis_index("var") * share_rows
    excess_sum, second_sum = lax.psum((excess_part, return_part), "smp")
    freq_next, freq_gradient = update_freqs(freqs, excess_sum, second_sum, sample_count)
    gradient_all, second_all = lax.psum((gradient_part, second_part), "var")
    fraction_next = normalize(fractions, gradient_all, second_all)
    own_next = lax.dynamic_slice_in_dim(fraction_next, first_row, share_rows, 0)
    own_gradient = lax.dynamic_slice_in_dim(gradient_all, first_row, share_rows, 0)
    scaled_gradient = own_gradient / math.sqrt(variant_count)
    ratio_next = dosage / jnp.dot(fraction_next, freqs, precision=highest)
    residual = residuals.astype(jnp.float32) / 1000.0
    trait_rows = (fraction_next[:, :, None] * residual[:, None, :]).reshape(
        sample_rows, anc_count * trait_count
    )
    score_part = jnp.dot(trait_rows.T, ratio_next, precision=highest)
    info_part = jnp.dot(
        (fraction_next * fraction_next).T, ratio_next * ratio_next, precision=highest
    )
    score_sum, info_sum = lax.psum((score_part, info_part), "smp")
    score_tiles = score_sum.reshape(anc_count, trait_count, genotypes.shape[1])
    z_score = score_tiles / jnp.sqrt(info_sum + 1e-06)[:, None, :]
    return (own_next, scaled_gradient, freq_next, freq_gradient, z_score)


def split(x):
    high = x.astype(BF16)
    return high, (x - high.astype(F32)).astype(BF16)


def dot(a, b):
    return jnp.dot(a, b, preferred_element_type=F32)


def dot_lanes(a, b):
    return lax.dot_general(a, b, (((1,), (1,)), ((), ())), preferred_element_type=F32)


def kernel(
    dims,
    geno_in, counts_in, resid_in, freqs_in,
    q_out, g_out, p_out, pg_out, z_out,
    geno, counts, resid, freqs, dos, qf, gf, fcol, frow, ebuf, tbuf,
    acc_ex, acc_sc, acc_in,
    xs, xr, zs, zr, go, gp, fs, fr, ss, sr,
    xs_s, xs_r, zs_s, zs_r, za_s, za_r, xa_s, xa_r, f_s, f_r, s_s, s_r, in_s,
):
    chunks, width, half, zs_n, rows, variant_count, sample_count, share, var_n = dims
    anc = freqs.shape[0]
    traits = resid.shape[0]
    mv = freqs.shape[1]
    me = lax.axis_index("var")
    core = lax.axis_index("smp")
    x = lax.rem(me, 2)
    z = me // 2
    partner = {"var": z * 2 + (1 - x)}
    twin = {"smp": 1 - core}
    z_peers = [{"var": lax.rem(z + d, zs_n) * 2 + x} for d in range(1, zs_n)]

    def load(src, dst, which, base=None, size=None):
        if base is not None:
            src, dst = src.at[pl.ds(base, size), :], dst.at[pl.ds(base, size), :]
        return pltpu.make_async_copy(src, dst, in_s.at[which])

    far_half = pl.multiple_of((1 - x) * half, 128)
    near_half = pl.multiple_of(x * half, 128)
    freqs_load = load(freqs_in, freqs, 0)
    counts_load = load(counts_in, counts, 1)
    far_load = load(geno_in, geno, 2, far_half, half)
    near_load = load(geno_in, geno, 3, near_half, half)
    resid_load = load(resid_in, resid, 4)
    for item in (freqs_load, counts_load, far_load, near_load, resid_load):
        item.start()

    barrier = pltpu.get_barrier_semaphore()
    for peer in [partner, twin] + z_peers:
        pl.semaphore_signal(barrier, inc=1, device_id=peer, device_id_type=MESH)

    freqs_load.wait()
    p = freqs[...]
    p_hi, p_lo = split(p)
    stack = jnp.concatenate([p_hi.astype(F32), p_lo.astype(F32)] * 2, axis=0)
    fcol[...] = stack.T.astype(BF16)
    frow[0:anc, 0:mv] = p_hi
    frow[0:anc, mv:] = p_hi
    frow[anc:, 0:mv] = p_lo
    frow[anc:, mv:] = p_lo
    acc_ex[...] = jnp.zeros_like(acc_ex)
    acc_sc[...] = jnp.zeros_like(acc_sc)
    acc_in[...] = jnp.zeros_like(acc_in)

    def lanes(which, c):
        return pl.multiple_of(which * half + c * width, 128)

    def first_pass(off):
        d = geno[pl.ds(off, width), :].astype(F32).T
        dos[:, pl.ds(off, width)] = d.astype(BF16)
        c = counts[:, pl.ds(off, width)].astype(F32)
        total = jnp.sum(c, axis=0, keepdims=True)
        cb = c.astype(BF16)
        none = jnp.zeros_like(cb)
        u = dot(fcol[...], jnp.concatenate([cb, cb, none, none], axis=0))
        w = total - u
        inverse = 1.0 / (u * w)
        b = (2.0 - d) * u * inverse
        e = d * w * inverse - b
        e_hi, e_lo = split(e)
        b_hi, b_lo = split(b)
        ebuf[0:mv, :] = e_hi
        ebuf[mv : 2 * mv, :] = e_lo
        ebuf[2 * mv : 3 * mv, :] = b_hi
        ebuf[3 * mv :, :] = b_lo
        g = dot(frow[...], ebuf[0 : 2 * mv, :])
        acc_ex[...] += dot_lanes(ebuf[...], jnp.concatenate([cb] * (128 // anc), axis=0))
        return (g[0:anc, :] + g[anc:, :]) * total

    def second_pass(off, g):
        c = counts[:, pl.ds(off, width)].astype(F32)
        f = c / jnp.sum(c, axis=0, keepdims=True)
        second = 2.0 * variant_count - jnp.sum(f * g, axis=0, keepdims=True)
        weighted = f * (g + second)
        q = weighted / jnp.sum(weighted, axis=0, keepdims=True)
        qf[:, pl.ds(off, width)] = q
        gf[:, pl.ds(off, width)] = g * (1.0 / math.sqrt(variant_count))
        q_hi, q_lo = split(q)
        recon = dot(fcol[...], jnp.concatenate([q_hi, q_hi, q_lo, q_lo], axis=0))
        r = dos[:, pl.ds(off, width)].astype(F32) / recon
        r_hi, r_lo = split(r)
        s_hi, s_lo = split(r * r)
        t = resid[:, pl.ds(off, width)].astype(F32)
        for k in range(anc):
            t_hi, t_lo = split(q[k : k + 1, :] * t)
            tbuf[traits * k : traits * (k + 1), 0:width] = t_hi
            tbuf[traits * k : traits * (k + 1), width:] = t_lo
        r_cat = jnp.concatenate([r_hi, r_lo], axis=0)
        acc_sc[...] += dot_lanes(tbuf[...], jnp.concatenate([r_cat, r_cat], axis=1))
        y_hi, y_lo = split(q * q)
        none = jnp.zeros_like(y_hi)
        acc_in[...] += dot_lanes(
            jnp.concatenate([s_hi, s_lo], axis=0),
            jnp.concatenate([y_hi, y_lo, none, none], axis=0),
        )

    def copy(src, dst, send, recv, peer):
        return pltpu.make_async_remote_copy(
            src_ref=src, dst_ref=dst, send_sem=send, recv_sem=recv, device_id=peer, device_id_type=MESH
        )

    def x_reduce(c):
        return copy(xs.at[c], xr.at[c], xs_s.at[c], xs_r.at[c], partner)

    def z_reduce(c, d):
        to = pl.multiple_of(lax.rem(z + d, zs_n) * rows, 8)
        return copy(
            zs.at[c, pl.ds(to, rows), :], zr.at[c, d - 1], zs_s.at[c, d - 1], zs_r.at[c, d - 1], z_peers[d - 1]
        )

    mine = pl.multiple_of(z * rows, 8)

    def z_gather(c, d):
        piece = go.at[c, pl.ds(mine, rows), :]
        return copy(piece, piece, za_s.at[c, d - 1], za_r.at[c, d - 1], z_peers[d - 1])

    def z_gathered(c, d):
        source = pl.multiple_of(lax.rem(z + zs_n - d, zs_n) * rows, 8)
        piece = go.at[c, pl.ds(source, rows), :]
        return copy(piece, piece, za_s.at[c, d - 1], za_r.at[c, d - 1], z_peers[d - 1])

    def x_gather(c):
        return copy(go.at[c], gp.at[c], xa_s.at[c], xa_r.at[c], partner)

    counts_load.wait()
    far_load.wait()
    xs[0] = first_pass(lanes(1 - x, 0))
    pl.semaphore_wait(barrier, 2 + len(z_peers))
    x_reduce(0).start()

    def step_far(c, carry):
        xs[c] = first_pass(lanes(1 - x, c))
        x_reduce(c).start()
        return carry

    lax.fori_loop(1, chunks, step_far, 0)
    near_load.wait()

    def step_near(c, carry):
        g = first_pass(lanes(x, c))
        x_reduce(c).wait_recv()
        zs[c] = g + xr[c]
        for d in range(1, zs_n):
            z_reduce(c, d).start()
        return carry

    lax.fori_loop(0, chunks, step_near, 0)

    ex = acc_ex[0:mv, :] + acc_ex[mv : 2 * mv, :]
    re = acc_ex[2 * mv : 3 * mv, :] + acc_ex[3 * mv :, :]
    fs[0:anc, :] = ex.T[0:anc, :]
    fs[anc:, :] = re.T[0:anc, :]
    freq_copy = copy(fs, fr, f_s, f_r, twin)
    freq_copy.start()

    def step_sum(c, carry):
        total = zs[c, pl.ds(mine, rows), :]
        for d in range(1, zs_n):
            z_reduce(c, d).wait_recv()
            total = total + zr[c, d - 1]
        go[c, pl.ds(mine, rows), :] = total
        for d in range(1, zs_n):
            z_gather(c, d).start()
        return carry

    lax.fori_loop(0, chunks, step_sum, 0)

    resid_load.wait()
    freq_copy.wait_recv()
    sums = fs[...] + fr[...]
    excess_sum = sums[0:anc, :]
    second_sum = sums[anc:, :]
    freq_next, freq_gradient = update_freqs(p, excess_sum, second_sum, sample_count)
    p_out[...] = freq_next
    pg_out[...] = freq_gradient

    def step_own(c, carry):
        for d in range(1, zs_n):
            z_gathered(c, d).wait_recv()
        x_gather(c).start()
        second_pass(lanes(x, c), go[c])
        return carry

    lax.fori_loop(0, chunks, step_own, 0)

    def step_other(c, carry):
        x_gather(c).wait_recv()
        second_pass(lanes(1 - x, c), gp[c])
        return carry

    lax.fori_loop(0, chunks, step_other, 0)

    tiles = anc * traits
    ss[0:tiles, :] = acc_sc[:, 0:mv] + acc_sc[:, mv:]
    info = (acc_in[0:mv, :] + acc_in[mv:, :]).T
    ss[tiles:, :] = info[0:anc, :] + info[anc : 2 * anc, :]
    score_copy = copy(ss, sr, s_s, s_r, twin)
    score_copy.start()

    for v in range(var_n):

        @pl.when(me == v)
        def _():
            q_out[...] = qf[:, share * v : share * (v + 1)]
            g_out[...] = gf[:, share * v : share * (v + 1)]

    def drain(c, carry):
        x_reduce(c).wait_send()
        x_gather(c).wait_send()
        for d in range(1, zs_n):
            z_reduce(c, d).wait_send()
            z_gather(c, d).wait_send()
        return carry

    lax.fori_loop(0, chunks, drain, 0)
    freq_copy.wait_send()
    score_copy.wait_recv()
    info_sum = ss[tiles:, :] + sr[tiles:, :]
    scale = 0.001 / jnp.sqrt(info_sum + 1e-06)
    for k in range(anc):
        at = slice(traits * k, traits * (k + 1))
        z_out[at, :] = (ss[at, :] + sr[at, :]) * scale[k : k + 1, :]
    score_copy.wait_send()


def store_kernel(*refs):
    count = len(refs) // 2
    sems = refs[-1]
    copies = [pltpu.make_async_copy(refs[i], refs[count + i], sems.at[i]) for i in range(count)]
    for item in copies:
        item.start()
    for item in copies:
        item.wait()


def store(*arrays):
    return pl.pallas_call(
        store_kernel,
        out_shape=tuple(jax.ShapeDtypeStruct(a.shape, a.dtype) for a in arrays),
        in_specs=[pl.BlockSpec(memory_space=pltpu.VMEM)] * len(arrays),
        out_specs=(pl.BlockSpec(memory_space=pl.ANY),) * len(arrays),
        scratch_shapes=[pltpu.SemaphoreType.DMA((len(arrays),))],
        compiler_params=pltpu.CompilerParams(vmem_limit_bytes=1024 * 1024),
        name="store",
    )(*arrays)


def fits(genotypes, residuals, freqs, var_n):
    samples, mv = genotypes.shape
    anc = freqs.shape[0]
    return (
        var_n == 8
        and lax.axis_size("smp") == 2
        and anc == 32
        and mv == 128
        and residuals.shape[1] % 16 == 0
        and samples % (2 * 128) == 0
        and samples % var_n == 0
    )


def shards(genotypes, ancestry_counts, residuals, freqs):
    var_n = lax.axis_size("var")
    if not fits(genotypes, residuals, freqs, var_n):
        return shards_plain(genotypes, ancestry_counts, residuals, freqs)
    samples, mv = genotypes.shape
    anc = freqs.shape[0]
    traits = residuals.shape[1]
    zs_n = var_n // 2
    rows = anc // zs_n
    half = samples // 2
    tiles = half // 128
    chunks = max(n for n in range(1, MOST + 1) if tiles % n == 0)
    width = half // chunks
    share = samples // var_n
    dims = (chunks, width, half, zs_n, rows, mv * var_n, samples * lax.axis_size("smp"), share, var_n)
    vmem = pl.BlockSpec(memory_space=pltpu.VMEM)
    dma = pltpu.SemaphoreType.DMA
    part = pltpu.VMEM((chunks, anc, width), F32)
    results = pl.pallas_call(
        functools.partial(kernel, dims),
        out_shape=(
            pltpu.VMEM((anc, share), F32),
            pltpu.VMEM((anc, share), F32),
            pltpu.VMEM((anc, mv), F32),
            pltpu.VMEM((anc, mv), F32),
            pltpu.VMEM((anc * traits, mv), F32),
        ),
        in_specs=[pl.BlockSpec(memory_space=pltpu.HBM)] * 4,
        out_specs=(vmem,) * 5,
        scratch_shapes=[
            pltpu.VMEM((samples, mv), BF16),
            pltpu.VMEM((anc, samples), jnp.int32),
            pltpu.VMEM((traits, samples), jnp.int32),
            pltpu.VMEM((anc, mv), F32),
            pltpu.VMEM((mv, samples), BF16),
            pltpu.VMEM((anc, samples), F32),
            pltpu.VMEM((anc, samples), F32),
            pltpu.VMEM((mv, 4 * anc), BF16),
            pltpu.VMEM((2 * anc, 2 * mv), BF16),
            pltpu.VMEM((4 * mv, width), BF16),
            pltpu.VMEM((anc * traits, 2 * width), BF16),
            pltpu.VMEM((4 * mv, 128), F32),
            pltpu.VMEM((anc * traits, 2 * mv), F32),
            pltpu.VMEM((2 * mv, 128), F32),
            part, part, part,
            pltpu.VMEM((chunks, zs_n - 1, rows, width), F32),
            part, part,
            pltpu.VMEM((2 * anc, mv), F32),
            pltpu.VMEM((2 * anc, mv), F32),
            pltpu.VMEM((anc * traits + anc, mv), F32),
            pltpu.VMEM((anc * traits + anc, mv), F32),
            dma((chunks,)), dma((chunks,)),
            dma((chunks, zs_n - 1)), dma((chunks, zs_n - 1)),
            dma((chunks, zs_n - 1)), dma((chunks, zs_n - 1)),
            dma((chunks,)), dma((chunks,)),
            dma, dma, dma, dma, dma((5,)),
        ],
        compiler_params=pltpu.CompilerParams(collective_id=0, has_side_effects=True, vmem_limit_bytes=LIMIT),
        name="em_step",
    )(genotypes, ancestry_counts.T, residuals.T, freqs)
    q_t, g_t, p_new, p_grad, z_flat = store(*results)
    return (q_t.T, g_t.T, p_new, p_grad, z_flat.reshape(anc, traits, mv))


def solution(mesh):
    in_specs = (
        P(("grp", "smp"), "var"),
        P(("grp", "smp"), None),
        P(("grp", "smp"), None),
        P("grp", "var"),
    )
    out_specs = (
        P(("grp", "smp", "var"), None),
        P(("grp", "smp", "var"), None),
        P("grp", "var"),
        P("grp", "var"),
        P("grp", None, "var"),
    )
    return jax.shard_map(shards, mesh=mesh, in_specs=in_specs, out_specs=out_specs, check_vma=False)
```

```python
import functools
import math

import jax
import jax.numpy as jnp
from jax import lax
from jax.experimental import pallas as pl
from jax.experimental.pallas import tpu as pltpu
from jax.sharding import PartitionSpec as P

MESH = pl.DeviceIdType.MESH
F32 = jnp.float32
BF16 = jnp.bfloat16
LIMIT = 67043328 - 491520
MOST = 5


def normalize(fractions, gradient, second):
    weighted = fractions * (gradient + second[:, None])
    return weighted / jnp.sum(weighted, axis=1, keepdims=True)


def update_freqs(freqs, excess_sum, second_sum, sample_count):
    allele_sum = excess_sum + second_sum
    freq_next = freqs * allele_sum / (freqs * allele_sum + (1.0 - freqs) * second_sum)
    freq_gradient = excess_sum * freqs.shape[0] / math.sqrt(sample_count)
    return (freq_next, freq_gradient)


def shards_plain(genotypes, ancestry_counts, residuals, freqs):
    highest = lax.Precision.HIGHEST
    var_count = lax.axis_size("var")
    sample_rows = genotypes.shape[0]
    sample_count = sample_rows * lax.axis_size("smp")
    variant_count = genotypes.shape[1] * var_count
    anc_count = freqs.shape[0]
    trait_count = residuals.shape[1]
    counts = ancestry_counts.astype(jnp.float32)
    fractions = counts / jnp.sum(counts, axis=1, keepdims=True)
    dosage = genotypes.astype(jnp.float32)
    recon_rows = jnp.dot(fractions, freqs, precision=highest)
    ratio_a = dosage / recon_rows
    ratio_b = (2.0 - dosage) / (1.0 - recon_rows)
    excess = ratio_a - ratio_b
    gradient_part = jnp.dot(excess, freqs.T, precision=highest)
    second_part = jnp.sum(ratio_b, axis=1)
    excess_part = jnp.dot(fractions.T, excess, precision=highest)
    return_part = jnp.dot(fractions.T, ratio_b, precision=highest)
    share_rows = sample_rows // var_count
    first_row = lax.axis_index("var") * share_rows
    excess_sum, second_sum = lax.psum((excess_part, return_part), "smp")
    freq_next, freq_gradient = update_freqs(freqs, excess_sum, second_sum, sample_count)
    gradient_all, second_all = lax.psum((gradient_part, second_part), "var")
    fraction_next = normalize(fractions, gradient_all, second_all)
    own_next = lax.dynamic_slice_in_dim(fraction_next, first_row, share_rows, 0)
    own_gradient = lax.dynamic_slice_in_dim(gradient_all, first_row, share_rows, 0)
    scaled_gradient = own_gradient / math.sqrt(variant_count)
    ratio_next = dosage / jnp.dot(fraction_next, freqs, precision=highest)
    residual = residuals.astype(jnp.float32) / 1000.0
    trait_rows = (fraction_next[:, :, None] * residual[:, None, :]).reshape(
        sample_rows, anc_count * trait_count
    )
    score_part = jnp.dot(trait_rows.T, ratio_next, precision=highest)
    info_part = jnp.dot(
        (fraction_next * fraction_next).T, ratio_next * ratio_next, precision=highest
    )
    score_sum, info_sum = lax.psum((score_part, info_part), "smp")
    score_tiles = score_sum.reshape(anc_count, trait_count, genotypes.shape[1])
    z_score = score_tiles / jnp.sqrt(info_sum + 1e-06)[:, None, :]
    return (own_next, scaled_gradient, freq_next, freq_gradient, z_score)


def split(x):
    high = x.astype(BF16)
    return high, (x - high.astype(F32)).astype(BF16)


def dot(a, b):
    return jnp.dot(a, b, preferred_element_type=F32)


def dot_lanes(a, b):
    return lax.dot_general(a, b, (((1,), (1,)), ((), ())), preferred_element_type=F32)


def kernel(
    dims,
    geno_in, counts_in, resid_in, freqs_in,
    q_out, g_out, p_out, pg_out, z_out,
    geno, counts, resid, freqs, dos, qf, gf, fcol, frow, ebuf, tbuf,
    acc_ex, acc_sc, acc_in,
    xs, xr, zs, zr, go, gp, fs, fr, ss, sr,
    xs_s, xs_r, zs_s, zs_r, za_s, za_r, xa_s, xa_r, f_s, f_r, s_s, s_r, in_s,
):
    chunks, width, half, zs_n, rows, variant_count, sample_count, share, var_n = dims
    anc = freqs.shape[0]
    traits = resid.shape[0]
    mv = freqs.shape[1]
    me = lax.axis_index("var")
    core = lax.axis_index("smp")
    x = lax.rem(me, 2)
    z = me // 2
    partner = {"var": z * 2 + (1 - x)}
    twin = {"smp": 1 - core}
    z_peers = [{"var": lax.rem(z + d, zs_n) * 2 + x} for d in range(1, zs_n)]

    def load(src, dst, which, base=None, size=None):
        if base is not None:
            src, dst = src.at[pl.ds(base, size), :], dst.at[pl.ds(base, size), :]
        return pltpu.make_async_copy(src, dst, in_s.at[which])

    far_half = pl.multiple_of((1 - x) * half, 128)
    near_half = pl.multiple_of(x * half, 128)
    freqs_load = load(freqs_in, freqs, 0)
    counts_load = load(counts_in, counts, 1)
    far_load = load(geno_in, geno, 2, far_half, half)
    near_load = load(geno_in, geno, 3, near_half, half)
    resid_load = load(resid_in, resid, 4)
    for item in (freqs_load, counts_load, far_load, near_load, resid_load):
        item.start()

    barrier = pltpu.get_barrier_semaphore()
    for peer in [partner, twin] + z_peers:
        pl.semaphore_signal(barrier, inc=1, device_id=peer, device_id_type=MESH)

    freqs_load.wait()
    p = freqs[...]
    p_hi, p_lo = split(p)
    stack = jnp.concatenate([p_hi.astype(F32), p_lo.astype(F32)] * 2, axis=0)
    fcol[...] = stack.T.astype(BF16)
    frow[0:anc, 0:mv] = p_hi
    frow[0:anc, mv:] = p_hi
    frow[anc:, 0:mv] = p_lo
    frow[anc:, mv:] = p_lo
    acc_ex[...] = jnp.zeros_like(acc_ex)
    acc_sc[...] = jnp.zeros_like(acc_sc)
    acc_in[...] = jnp.zeros_like(acc_in)

    def lanes(which, c):
        return pl.multiple_of(which * half + c * width, 128)

    def first_pass(off):
        d = geno[pl.ds(off, width), :].astype(F32).T
        dos[:, pl.ds(off, width)] = d.astype(BF16)
        c = counts[:, pl.ds(off, width)].astype(F32)
        total = jnp.sum(c, axis=0, keepdims=True)
        cb = c.astype(BF16)
        none = jnp.zeros_like(cb)
        u = dot(fcol[...], jnp.concatenate([cb, cb, none, none], axis=0))
        w = total - u
        inverse = 1.0 / (u * w)
        b = (2.0 - d) * u * inverse
        e = d * w * inverse - b
        e_hi, e_lo = split(e)
        b_hi, b_lo = split(b)
        ebuf[0:mv, :] = e_hi
        ebuf[mv : 2 * mv, :] = e_lo
        ebuf[2 * mv : 3 * mv, :] = b_hi
        ebuf[3 * mv :, :] = b_lo
        g = dot(frow[...], ebuf[0 : 2 * mv, :])
        acc_ex[...] += dot_lanes(ebuf[...], jnp.concatenate([cb] * (128 // anc), axis=0))
        return (g[0:anc, :] + g[anc:, :]) * total

    def second_pass(off, g):
        c = counts[:, pl.ds(off, width)].astype(F32)
        f = c / jnp.sum(c, axis=0, keepdims=True)
        second = 2.0 * variant_count - jnp.sum(f * g, axis=0, keepdims=True)
        weighted = f * (g + second)
        q = weighted / jnp.sum(weighted, axis=0, keepdims=True)
        qf[:, pl.ds(off, width)] = q
        gf[:, pl.ds(off, width)] = g * (1.0 / math.sqrt(variant_count))
        q_hi, q_lo = split(q)
        recon = dot(fcol[...], jnp.concatenate([q_hi, q_hi, q_lo, q_lo], axis=0))
        r = dos[:, pl.ds(off, width)].astype(F32) / recon
        r_hi, r_lo = split(r)
        s_hi, s_lo = split(r * r)
        t = resid[:, pl.ds(off, width)].astype(F32)
        for k in range(anc):
            t_hi, t_lo = split(q[k : k + 1, :] * t)
            tbuf[traits * k : traits * (k + 1), 0:width] = t_hi
            tbuf[traits * k : traits * (k + 1), width:] = t_lo
        r_cat = jnp.concatenate([r_hi, r_lo], axis=0)
        acc_sc[...] += dot_lanes(tbuf[...], jnp.concatenate([r_cat, r_cat], axis=1))
        y_hi, y_lo = split(q * q)
        none = jnp.zeros_like(y_hi)
        acc_in[...] += dot_lanes(
            jnp.concatenate([s_hi, s_lo], axis=0),
            jnp.concatenate([y_hi, y_lo, none, none], axis=0),
        )

    def copy(src, dst, send, recv, peer):
        return pltpu.make_async_remote_copy(
            src_ref=src, dst_ref=dst, send_sem=send, recv_sem=recv, device_id=peer, device_id_type=MESH
        )

    def x_reduce(c):
        return copy(xs.at[c], xr.at[c], xs_s.at[c], xs_r.at[c], partner)

    def z_reduce(c, d):
        to = pl.multiple_of(lax.rem(z + d, zs_n) * rows, 8)
        return copy(
            zs.at[c, pl.ds(to, rows), :], zr.at[c, d - 1], zs_s.at[c, d - 1], zs_r.at[c, d - 1], z_peers[d - 1]
        )

    mine = pl.multiple_of(z * rows, 8)

    def z_gather(c, d):
        piece = go.at[c, pl.ds(mine, rows), :]
        return copy(piece, piece, za_s.at[c, d - 1], za_r.at[c, d - 1], z_peers[d - 1])

    def z_gathered(c, d):
        source = pl.multiple_of(lax.rem(z + zs_n - d, zs_n) * rows, 8)
        piece = go.at[c, pl.ds(source, rows), :]
        return copy(piece, piece, za_s.at[c, d - 1], za_r.at[c, d - 1], z_peers[d - 1])

    def x_gather(c, d):
        source = pl.multiple_of(lax.rem(z + zs_n - d, zs_n) * rows, 8)
        return copy(
            go.at[c, pl.ds(source, rows), :], gp.at[c, pl.ds(source, rows), :], xa_s.at[c, d], xa_r.at[c, d], partner
        )

    counts_load.wait()
    far_load.wait()
    xs[0] = first_pass(lanes(1 - x, 0))
    pl.semaphore_wait(barrier, 2 + len(z_peers))
    x_reduce(0).start()

    def step_far(c, carry):
        xs[c] = first_pass(lanes(1 - x, c))
        x_reduce(c).start()
        return carry

    lax.fori_loop(1, chunks, step_far, 0)
    near_load.wait()

    def step_near(c, carry):
        g = first_pass(lanes(x, c))
        x_reduce(c).wait_recv()
        zs[c] = g + xr[c]
        for d in range(1, zs_n):
            z_reduce(c, d).start()
        return carry

    lax.fori_loop(0, chunks, step_near, 0)

    ex = acc_ex[0:mv, :] + acc_ex[mv : 2 * mv, :]
    re = acc_ex[2 * mv : 3 * mv, :] + acc_ex[3 * mv :, :]
    fs[0:anc, :] = ex.T[0:anc, :]
    fs[anc:, :] = re.T[0:anc, :]
    freq_copy = copy(fs, fr, f_s, f_r, twin)
    freq_copy.start()

    def step_sum(c, carry):
        total = zs[c, pl.ds(mine, rows), :]
        for d in range(1, zs_n):
            z_reduce(c, d).wait_recv()
            total = total + zr[c, d - 1]
        go[c, pl.ds(mine, rows), :] = total
        for d in range(1, zs_n):
            z_gather(c, d).start()
        x_gather(c, 0).start()
        return carry

    lax.fori_loop(0, chunks, step_sum, 0)

    resid_load.wait()
    freq_copy.wait_recv()
    sums = fs[...] + fr[...]
    excess_sum = sums[0:anc, :]
    second_sum = sums[anc:, :]
    freq_next, freq_gradient = update_freqs(p, excess_sum, second_sum, sample_count)
    p_out[...] = freq_next
    pg_out[...] = freq_gradient

    def step_own(c, carry):
        for d in range(1, zs_n):
            z_gathered(c, d).wait_recv()
            x_gather(c, d).start()
        second_pass(lanes(x, c), go[c])
        return carry

    lax.fori_loop(0, chunks, step_own, 0)

    def step_other(c, carry):
        for d in range(zs_n):
            x_gather(c, d).wait_recv()
        second_pass(lanes(1 - x, c), gp[c])
        return carry

    lax.fori_loop(0, chunks, step_other, 0)

    tiles = anc * traits
    ss[0:tiles, :] = acc_sc[:, 0:mv] + acc_sc[:, mv:]
    info = (acc_in[0:mv, :] + acc_in[mv:, :]).T
    ss[tiles:, :] = info[0:anc, :] + info[anc : 2 * anc, :]
    score_copy = copy(ss, sr, s_s, s_r, twin)
    score_copy.start()

    for v in range(var_n):

        @pl.when(me == v)
        def _():
            q_out[...] = qf[:, share * v : share * (v + 1)]
            g_out[...] = gf[:, share * v : share * (v + 1)]

    def drain(c, carry):
        x_reduce(c).wait_send()
        for d in range(zs_n):
            x_gather(c, d).wait_send()
        for d in range(1, zs_n):
            z_reduce(c, d).wait_send()
            z_gather(c, d).wait_send()
        return carry

    lax.fori_loop(0, chunks, drain, 0)
    freq_copy.wait_send()
    score_copy.wait_recv()
    info_sum = ss[tiles:, :] + sr[tiles:, :]
    scale = 0.001 / jnp.sqrt(info_sum + 1e-06)
    for k in range(anc):
        at = slice(traits * k, traits * (k + 1))
        z_out[at, :] = (ss[at, :] + sr[at, :]) * scale[k : k + 1, :]
    score_copy.wait_send()


def store_kernel(*refs):
    count = len(refs) // 2
    sems = refs[-1]
    copies = [pltpu.make_async_copy(refs[i], refs[count + i], sems.at[i]) for i in range(count)]
    for item in copies:
        item.start()
    for item in copies:
        item.wait()


def store(*arrays):
    return pl.pallas_call(
        store_kernel,
        out_shape=tuple(jax.ShapeDtypeStruct(a.shape, a.dtype) for a in arrays),
        in_specs=[pl.BlockSpec(memory_space=pltpu.VMEM)] * len(arrays),
        out_specs=(pl.BlockSpec(memory_space=pl.ANY),) * len(arrays),
        scratch_shapes=[pltpu.SemaphoreType.DMA((len(arrays),))],
        compiler_params=pltpu.CompilerParams(vmem_limit_bytes=1024 * 1024),
        name="store",
    )(*arrays)


def fits(genotypes, residuals, freqs, var_n):
    samples, mv = genotypes.shape
    anc = freqs.shape[0]
    return (
        var_n == 8
        and lax.axis_size("smp") == 2
        and anc == 32
        and mv == 128
        and residuals.shape[1] % 16 == 0
        and samples % (2 * 128) == 0
        and samples % var_n == 0
    )


def shards(genotypes, ancestry_counts, residuals, freqs):
    var_n = lax.axis_size("var")
    if not fits(genotypes, residuals, freqs, var_n):
        return shards_plain(genotypes, ancestry_counts, residuals, freqs)
    samples, mv = genotypes.shape
    anc = freqs.shape[0]
    traits = residuals.shape[1]
    zs_n = var_n // 2
    rows = anc // zs_n
    half = samples // 2
    tiles = half // 128
    chunks = max(n for n in range(1, MOST + 1) if tiles % n == 0)
    width = half // chunks
    share = samples // var_n
    dims = (chunks, width, half, zs_n, rows, mv * var_n, samples * lax.axis_size("smp"), share, var_n)
    vmem = pl.BlockSpec(memory_space=pltpu.VMEM)
    dma = pltpu.SemaphoreType.DMA
    part = pltpu.VMEM((chunks, anc, width), F32)
    results = pl.pallas_call(
        functools.partial(kernel, dims),
        out_shape=(
            pltpu.VMEM((anc, share), F32),
            pltpu.VMEM((anc, share), F32),
            pltpu.VMEM((anc, mv), F32),
            pltpu.VMEM((anc, mv), F32),
            pltpu.VMEM((anc * traits, mv), F32),
        ),
        in_specs=[pl.BlockSpec(memory_space=pltpu.HBM)] * 4,
        out_specs=(vmem,) * 5,
        scratch_shapes=[
            pltpu.VMEM((samples, mv), BF16),
            pltpu.VMEM((anc, samples), jnp.int32),
            pltpu.VMEM((traits, samples), jnp.int32),
            pltpu.VMEM((anc, mv), F32),
            pltpu.VMEM((mv, samples), BF16),
            pltpu.VMEM((anc, samples), F32),
            pltpu.VMEM((anc, samples), F32),
            pltpu.VMEM((mv, 4 * anc), BF16),
            pltpu.VMEM((2 * anc, 2 * mv), BF16),
            pltpu.VMEM((4 * mv, width), BF16),
            pltpu.VMEM((anc * traits, 2 * width), BF16),
            pltpu.VMEM((4 * mv, 128), F32),
            pltpu.VMEM((anc * traits, 2 * mv), F32),
            pltpu.VMEM((2 * mv, 128), F32),
            part, part, part,
            pltpu.VMEM((chunks, zs_n - 1, rows, width), F32),
            part, part,
            pltpu.VMEM((2 * anc, mv), F32),
            pltpu.VMEM((2 * anc, mv), F32),
            pltpu.VMEM((anc * traits + anc, mv), F32),
            pltpu.VMEM((anc * traits + anc, mv), F32),
            dma((chunks,)), dma((chunks,)),
            dma((chunks, zs_n - 1)), dma((chunks, zs_n - 1)),
            dma((chunks, zs_n - 1)), dma((chunks, zs_n - 1)),
            dma((chunks, zs_n)), dma((chunks, zs_n)),
            dma, dma, dma, dma, dma((5,)),
        ],
        compiler_params=pltpu.CompilerParams(collective_id=0, has_side_effects=True, vmem_limit_bytes=LIMIT),
        name="em_step",
    )(genotypes, ancestry_counts.T, residuals.T, freqs)
    q_t, g_t, p_new, p_grad, z_flat = store(*results)
    return (q_t.T, g_t.T, p_new, p_grad, z_flat.reshape(anc, traits, mv))


def solution(mesh):
    in_specs = (
        P(("grp", "smp"), "var"),
        P(("grp", "smp"), None),
        P(("grp", "smp"), None),
        P("grp", "var"),
    )
    out_specs = (
        P(("grp", "smp", "var"), None),
        P(("grp", "smp", "var"), None),
        P("grp", "var"),
        P("grp", "var"),
        P("grp", None, "var"),
    )
    return jax.shard_map(shards, mesh=mesh, in_specs=in_specs, out_specs=out_specs, check_vma=False)
```
